8 devices in a mesh: data: 2 (over z, y), tp: 4 (over x, core).
Axes of the slice: x: 2, y: 2, z: 1, core: 2. Of those that a mesh axis runs over, the one named last changes fastest.
Arguments:
- x_one: bfloat16 [1024, 49152], P('data', 'tp'), parts along dimension 0
- x_two: bfloat16 [1024, 49152], P('data', 'tp'), parts along dimension 0
- w_down: bfloat16 [49152, 12288], P('tp')
Outputs:
- output 1: bfloat16 [1024, 12288], P('data'), parts along dimension 0
- output 2: bfloat16 [1024, 12288], P('data'), parts along dimension 0
There are 2 independent parts. The reference program is written for one: setup_inputs(seed, part) draws one part's arguments, and reference() takes and returns one part's arrays. A program takes and returns all parts, laid end to end along the dimension named above; an argument that names none is the same for every part.
All inputs are finite; a program needn't handle non-finite values.
Results may differ from the reference program's by a relative error of at most 0.001.
Values are sent between devices in bfloat16 or wider.
A program may use at most 1.5 GiB of HBM per device.

```python
import jax
import jax.numpy as jnp

F = 49152
H = 12288
MB = 512


def setup_inputs(seed: int = 0, part: int = 0) -> dict:
    base_key = jax.random.key(seed)
    part_key = jax.random.fold_in(base_key, part)
    x_one = jax.random.normal(jax.random.fold_in(part_key, 1), (MB, F), jnp.float32).astype(jnp.bfloat16)
    x_two = jax.random.normal(jax.random.fold_in(part_key, 2), (MB, F), jnp.float32).astype(jnp.bfloat16)
    w_down = (jax.random.normal(jax.random.fold_in(base_key, 3), (F, H), jnp.float32) * (F ** -0.5)).astype(jnp.bfloat16)
    return {"x_one": x_one, "x_two": x_two, "w_down": w_down}


def reference(x_one, x_two, w_down):
    y_one = jnp.dot(x_one, w_down, preferred_element_type=jnp.float32).astype(jnp.bfloat16)
    y_two = jnp.dot(x_two, w_down, preferred_element_type=jnp.float32).astype(jnp.bfloat16)
    return (y_one, y_two)
```

```python
import functools

import jax
import jax.numpy as jnp
from jax import lax
from jax.experimental import pallas as pl
from jax.experimental.pallas import tpu as pltpu
from jax.sharding import PartitionSpec as P

MESH = pl.DeviceIdType.MESH
LEAD = 3
BN = 256
KC = 6


def kernel(
    x_one, x_two, w, y_one, y_two,
    xbuf, wbuf, acc, pair, part, own, peer, total,
    x_sem, w_sem, pair_send, pair_recv, part_send, part_recv,
    y_local, y_pair_send, y_pair_recv, y_send, y_recv, fwd_send, fwd_recv,
):
    rows, width = x_one.shape
    cols = w.shape[1]
    kb = width // KC
    np_ = cols // BN // 2
    steps = 2 * np_
    big = 2 * steps
    n_part, n_peer, n_total = part.shape[0], peer.shape[0], total.shape[0]

    t = lax.axis_index("tp")
    chip, lane = lax.div(t, 2), lax.rem(t, 2)
    sibling = {"tp": 2 * chip + 1 - lane}
    across = {"tp": 2 * (1 - chip) + lane}

    def at_least(s, a):
        return lax.div(s + big - a, big)

    def is_peer(s):
        head = 1 - at_least(s, LEAD)
        tail = at_least(s, steps - LEAD)
        return head + (1 - head - tail) * lax.rem(s + LEAD + 2, 2)

    def index(s):
        head = 1 - at_least(s, LEAD)
        tail = at_least(s, steps - LEAD)
        mid = 1 - head - tail
        odd = lax.rem(s + LEAD + 2, 2)
        u = s - LEAD + big
        return head * s + tail * (s - np_) + mid * (lax.div(u, 2) - big // 2 + odd * LEAD)

    def columns(owner, j):
        return pl.ds(pl.multiple_of((owner * np_ + j) * BN, BN), BN)

    def block_columns(s):
        p = is_peer(s)
        return columns(chip + p * (1 - 2 * chip), index(s))

    def w_copy(s, k):
        return pltpu.make_async_copy(
            w.at[pl.ds(k * kb, kb), block_columns(s)], wbuf.at[k], w_sem.at[k]
        )

    def x_copy(k, m):
        x = (x_one, x_two)[m]
        return pltpu.make_async_copy(
            x.at[:, pl.ds(k * kb, kb)], xbuf.at[k, pl.ds(m * rows, rows)], x_sem.at[m, k]
        )

    def half(slot, which):
        return acc.at[slot, pl.ds(pl.multiple_of(which * rows, rows), rows)]

    def pair_copy(s):
        slot = lax.rem(s, 2)
        return pltpu.make_async_remote_copy(
            half(slot, 1 - lane), pair.at[slot], pair_send.at[slot], pair_recv.at[slot],
            device_id=sibling, device_id_type=MESH,
        )

    def part_copy(j):
        a, b = lax.rem(j, n_part), lax.rem(j, n_peer)
        return pltpu.make_async_remote_copy(
            part.at[a], peer.at[b], part_send.at[a], part_recv.at[b],
            device_id=across, device_id_type=MESH,
        )

    def y_copies(y, j):
        a = lax.rem(j, n_total)
        dst = y.at[:, columns(chip, j)]
        return (
            pltpu.make_async_remote_copy(
                total.at[a], dst, y_send.at[a], y_recv.at[j],
                device_id=across, device_id_type=MESH,
            ),
            pltpu.make_async_remote_copy(
                total.at[a], dst, y_pair_send.at[a], y_pair_recv.at[j],
                device_id=sibling, device_id_type=MESH,
            ),
            pltpu.make_async_copy(total.at[a], dst, y_local.at[a]),
        )

    def fwd_copy(y, j):
        ref = y.at[:, columns(1 - chip, j)]
        return pltpu.make_async_remote_copy(
            ref, ref, fwd_send.at[j], fwd_recv.at[j], device_id=sibling, device_id_type=MESH
        )

    def by_lane(f):
        @pl.when(lane == 0)
        def _():
            f(y_one)

        @pl.when(lane == 1)
        def _():
            f(y_two)

    def add_pair(s):
        slot = lax.rem(s, 2)
        p, j = is_peer(s), index(s)
        pair_copy(s).wait()

        @pl.when(p == 1)
        def _():
            @pl.when(j >= n_part)
            def _():
                part_copy(j - n_part).wait_send()

            part[lax.rem(j, n_part)] = half(slot, lane)[...] + pair[slot]

        @pl.when(p == 0)
        def _():
            own[lax.rem(j, 2)] = half(slot, lane)[...] + pair[slot]

    def send_part(s):
        @pl.when(is_peer(s) == 1)
        def _():
            part_copy(index(s)).start()

    def finish(j):
        part_copy(j).wait_recv()

        @pl.when(j >= n_total)
        def _():
            for c in y_copies(y_one, j - n_total)[:2]:
                c.wait_send()
            y_copies(y_one, j - n_total)[2].wait()

        total[lax.rem(j, n_total)] = (
            own[lax.rem(j, 2)] + peer[lax.rem(j, n_peer)]
        ).astype(jnp.bfloat16)

    def send_total(j):
        by_lane(lambda y: [c.start() for c in y_copies(y, j)] and None)

    def forward(j):
        y_copies(y_one, j)[0].wait_recv()
        by_lane(lambda y: fwd_copy(y, j).start())

    for k in range(KC):
        x_copy(k, 0).start()
        x_copy(k, 1).start()
        w_copy(0, k).start()

    barrier = pltpu.get_barrier_semaphore()
    for other in (sibling, across):
        pl.semaphore_signal(barrier, inc=1, device_id=other, device_id_type=MESH)
    pl.semaphore_wait(barrier, 2)

    def step(s, carry):
        slot = lax.rem(s, 2)
        before = jnp.maximum(s - 2, 0)

        def own_two_back(f):
            @pl.when(s >= 2)
            def _():
                @pl.when(is_peer(before) == 0)
                def _():
                    f(index(before))

        for k in range(KC):
            @pl.when(s == 0)
            def _():
                x_copy(k, 0).wait()
                x_copy(k, 1).wait()

            w_copy(s, k).wait()
            product = jnp.dot(xbuf[k], wbuf[k], preferred_element_type=jnp.float32)
            if k == 0:
                acc[slot] = product
            else:
                acc[slot] += product

            @pl.when(s + 1 < steps)
            def _():
                w_copy(s + 1, k).start()

            if k == 0:
                @pl.when(s >= 1)
                def _():
                    pair_copy(s - 1).start()
            if k == 2:
                @pl.when(s >= 1)
                def _():
                    add_pair(s - 1)
            if k == 3:
                @pl.when(s >= 1)
                def _():
                    send_part(s - 1)

                own_two_back(finish)
            if k == 4:
                own_two_back(send_total)
            if k == 5:
                @pl.when(s >= 2)
                def _():
                    @pl.when(is_peer(before) == 0)
                    def _():
                        @pl.when(index(before) >= LEAD + 1)
                        def _():
                            forward(index(before) - LEAD - 1)
        return carry

    lax.fori_loop(0, steps, step, 0)

    last = steps - 1
    pair_copy(last).start()
    finish(np_ - 2)
    send_total(np_ - 2)
    add_pair(last)
    finish(np_ - 1)
    send_total(np_ - 1)
    for j in range(np_ - 2 - LEAD - 1, np_):
        forward(j)

    for j in range(np_ - n_part, np_):
        part_copy(j).wait_send()
    for j in range(np_ - n_total, np_):
        for c in y_copies(y_one, j)[:2]:
            c.wait_send()
        y_copies(y_one, j)[2].wait()

    def drain(j, carry):
        y_copies(y_one, j)[1].wait_recv()
        fwd_copy(y_one, j).wait()
        return carry

    lax.fori_loop(0, np_, drain, 0)


def solution(mesh):
    def per_device(x_one, x_two, w_down):
        rows, width = x_one.shape
        cols = w_down.shape[1]
        blocks = cols // BN // 2
        n_part, n_peer, n_total = LEAD + 2, 2 * LEAD + 2, LEAD + 2
        dma = pltpu.SemaphoreType.DMA
        out = jax.ShapeDtypeStruct((rows, cols), jnp.bfloat16)
        any_ = pl.BlockSpec(memory_space=pl.ANY)
        return pl.pallas_call(
            kernel,
            out_shape=(out, out),
            in_specs=[any_] * 3,
            out_specs=(any_, any_),
            scratch_shapes=[
                pltpu.VMEM((KC, 2 * rows, width // KC), jnp.bfloat16),
                pltpu.VMEM((KC, width // KC, BN), jnp.bfloat16),
                pltpu.VMEM((2, 2 * rows, BN), jnp.float32),
                pltpu.VMEM((2, rows, BN), jnp.float32),
                pltpu.VMEM((n_part, rows, BN), jnp.float32),
                pltpu.VMEM((2, rows, BN), jnp.float32),
                pltpu.VMEM((n_peer, rows, BN), jnp.float32),
                pltpu.VMEM((n_total, rows, BN), jnp.bfloat16),
                dma((2, KC)),
                dma((KC,)),
                dma((2,)),
                dma((2,)),
                dma((n_part,)),
                dma((n_peer,)),
                dma((n_total,)),
                dma((n_total,)),
                dma((blocks,)),
                dma((n_total,)),
                dma((blocks,)),
                dma((blocks,)),
                dma((blocks,)),
            ],
            compiler_params=pltpu.CompilerParams(
                collective_id=0, has_side_effects=True, vmem_limit_bytes=58 * 1024 * 1024
            ),
            cost_estimate=pl.CostEstimate(
                flops=4 * rows * width * cols,
                bytes_accessed=2 * width * cols,
                transcendentals=0,
            ),
        )(x_one, x_two, w_down)

    return jax.shard_map(
        per_device,
        mesh=mesh,
        in_specs=(P("data", "tp"), P("data", "tp"), P("tp", None)),
        out_specs=(P("data", None), P("data", None)),
        check_vma=False,
    )
```

```python
import functools

import jax
import jax.numpy as jnp
from jax import lax
from jax.experimental import pallas as pl
from jax.experimental.pallas import tpu as pltpu
from jax.sharding import PartitionSpec as P

MESH = pl.DeviceIdType.MESH
LEAD = 3
BN = 256
KC = 6


def kernel(
    x_one, x_two, w, y_one, y_two,
    xbuf, wbuf, acc, pair, part, own, peer, total,
    x_sem, w_sem, pair_send, pair_recv, part_send, part_recv,
    y_local, y_pair_send, y_pair_recv, y_send, y_recv, fwd_send, fwd_recv,
):
    rows, width = x_one.shape
    cols = w.shape[1]
    kb = width // KC
    np_ = cols // BN // 2
    steps = 2 * np_
    big = 2 * steps
    n_part, n_peer, n_total = part.shape[0], peer.shape[0], total.shape[0]

    t = lax.axis_index("tp")
    chip, lane = lax.div(t, 2), lax.rem(t, 2)
    sibling = {"tp": 2 * chip + 1 - lane}
    across = {"tp": 2 * (1 - chip) + lane}

    def at_least(s, a):
        return lax.div(s + big - a, big)

    def is_peer(s):
        head = 1 - at_least(s, LEAD)
        tail = at_least(s, steps - LEAD)
        return head + (1 - head - tail) * lax.rem(s + LEAD + 2, 2)

    def index(s):
        head = 1 - at_least(s, LEAD)
        tail = at_least(s, steps - LEAD)
        mid = 1 - head - tail
        odd = lax.rem(s + LEAD + 2, 2)
        u = s - LEAD + big
        return head * s + tail * (s - np_) + mid * (lax.div(u, 2) - big // 2 + odd * LEAD)

    def columns(owner, j):
        return pl.ds(pl.multiple_of((owner * np_ + j) * BN, BN), BN)

    def block_columns(s):
        p = is_peer(s)
        return columns(chip + p * (1 - 2 * chip), index(s))

    def w_copy(s, k):
        return pltpu.make_async_copy(
            w.at[pl.ds(k * kb, kb), block_columns(s)], wbuf.at[k], w_sem.at[k]
        )

    def x_copy(k, m):
        x = (x_one, x_two)[m]
        return pltpu.make_async_copy(
            x.at[:, pl.ds(k * kb, kb)], xbuf.at[k, pl.ds(m * rows, rows)], x_sem.at[m, k]
        )

    def half(slot, which):
        return acc.at[slot, pl.ds(pl.multiple_of(which * rows, rows), rows)]

    def pair_copy(s):
        slot = lax.rem(s, 2)
        return pltpu.make_async_remote_copy(
            half(slot, 1 - lane), pair.at[slot], pair_send.at[slot], pair_recv.at[slot],
            device_id=sibling, device_id_type=MESH,
        )

    def part_copy(j):
        a, b = lax.rem(j, n_part), lax.rem(j, n_peer)
        return pltpu.make_async_remote_copy(
            part.at[a], peer.at[b], part_send.at[a], part_recv.at[b],
            device_id=across, device_id_type=MESH,
        )

    def y_copies(y, j):
        a = lax.rem(j, n_total)
        dst = y.at[:, columns(chip, j)]
        return (
            pltpu.make_async_remote_copy(
                total.at[a], dst, y_send.at[a], y_recv.at[j],
                device_id=across, device_id_type=MESH,
            ),
            pltpu.make_async_remote_copy(
                total.at[a], dst, y_pair_send.at[a], y_pair_recv.at[j],
                device_id=sibling, device_id_type=MESH,
            ),
            pltpu.make_async_copy(total.at[a], dst, y_local.at[a]),
        )

    def fwd_copy(y, j):
        ref = y.at[:, columns(1 - chip, j)]
        return pltpu.make_async_remote_copy(
            ref, ref, fwd_send.at[j], fwd_recv.at[j], device_id=sibling, device_id_type=MESH
        )

    def by_lane(f):
        @pl.when(lane == 0)
        def _():
            f(y_one)

        @pl.when(lane == 1)
        def _():
            f(y_two)

    def add_pair(s):
        slot = lax.rem(s, 2)
        p, j = is_peer(s), index(s)
        pair_copy(s).wait()

        @pl.when(p == 1)
        def _():
            @pl.when(j >= n_part)
            def _():
                part_copy(j - n_part).wait_send()

            part[lax.rem(j, n_part)] = half(slot, lane)[...] + pair[slot]

        @pl.when(p == 0)
        def _():
            own[lax.rem(j, 2)] = half(slot, lane)[...] + pair[slot]

    def send_part(s):
        @pl.when(is_peer(s) == 1)
        def _():
            part_copy(index(s)).start()

    def finish(j):
        part_copy(j).wait_recv()

        @pl.when(j >= n_total)
        def _():
            for c in y_copies(y_one, j - n_total)[:2]:
                c.wait_send()
            y_copies(y_one, j - n_total)[2].wait()

        total[lax.rem(j, n_total)] = (
            own[lax.rem(j, 2)] + peer[lax.rem(j, n_peer)]
        ).astype(jnp.bfloat16)

    def send_total(j):
        by_lane(lambda y: [c.start() for c in y_copies(y, j)] and None)

    def forward(j):
        y_copies(y_one, j)[0].wait_recv()
        by_lane(lambda y: fwd_copy(y, j).start())

    for k in range(KC):
        x_copy(k, 0).start()
        x_copy(k, 1).start()
        w_copy(0, k).start()

    barrier = pltpu.get_barrier_semaphore()
    for other in (sibling, across):
        pl.semaphore_signal(barrier, inc=1, device_id=other, device_id_type=MESH)
    pl.semaphore_wait(barrier, 2)

    def step(s, carry):
        slot = lax.rem(s, 2)
        before = jnp.maximum(s - 2, 0)

        def own_two_back(f):
            @pl.when(s >= 2)
            def _():
                @pl.when(is_peer(before) == 0)
                def _():
                    f(index(before))

        for k in range(KC):
            @pl.when(s == 0)
            def _():
                x_copy(k, 0).wait()
                x_copy(k, 1).wait()

            w_copy(s, k).wait()
            for m in range(2):
                product = jnp.dot(xbuf[k, m * rows : (m + 1) * rows], wbuf[k], preferred_element_type=jnp.float32)
                if k == 0:
                    acc[slot, m * rows : (m + 1) * rows] = product
                else:
                    acc[slot, m * rows : (m + 1) * rows] += product

            @pl.when(s + 1 < steps)
            def _():
                w_copy(s + 1, k).start()

            if k == 0:
                @pl.when(s >= 1)
                def _():
                    pair_copy(s - 1).start()
            if k == 2:
                @pl.when(s >= 1)
                def _():
                    add_pair(s - 1)
            if k == 3:
                @pl.when(s >= 1)
                def _():
                    send_part(s - 1)

                own_two_back(finish)
            if k == 4:
                own_two_back(send_total)
            if k == 5:
                @pl.when(s >= 2)
                def _():
                    @pl.when(is_peer(before) == 0)
                    def _():
                        @pl.when(index(before) >= LEAD + 1)
                        def _():
                            forward(index(before) - LEAD - 1)
        return carry

    lax.fori_loop(0, steps, step, 0)

    last = steps - 1
    pair_copy(last).start()
    finish(np_ - 2)
    send_total(np_ - 2)
    add_pair(last)
    finish(np_ - 1)
    send_total(np_ - 1)
    for j in range(np_ - 2 - LEAD - 1, np_):
        forward(j)

    for j in range(np_ - n_part, np_):
        part_copy(j).wait_send()
    for j in range(np_ - n_total, np_):
        for c in y_copies(y_one, j)[:2]:
            c.wait_send()
        y_copies(y_one, j)[2].wait()

    def drain(j, carry):
        y_copies(y_one, j)[1].wait_recv()
        fwd_copy(y_one, j).wait()
        return carry

    lax.fori_loop(0, np_, drain, 0)


def solution(mesh):
    def per_device(x_one, x_two, w_down):
        rows, width = x_one.shape
        cols = w_down.shape[1]
        blocks = cols // BN // 2
        n_part, n_peer, n_total = LEAD + 2, 2 * LEAD + 2, LEAD + 2
        dma = pltpu.SemaphoreType.DMA
        out = jax.ShapeDtypeStruct((rows, cols), jnp.bfloat16)
        any_ = pl.BlockSpec(memory_space=pl.ANY)
        return pl.pallas_call(
            kernel,
            out_shape=(out, out),
            in_specs=[any_] * 3,
            out_specs=(any_, any_),
            scratch_shapes=[
                pltpu.VMEM((KC, 2 * rows, width // KC), jnp.bfloat16),
                pltpu.VMEM((KC, width // KC, BN), jnp.bfloat16),
                pltpu.VMEM((2, 2 * rows, BN), jnp.float32),
                pltpu.VMEM((2, rows, BN), jnp.float32),
                pltpu.VMEM((n_part, rows, BN), jnp.float32),
                pltpu.VMEM((2, rows, BN), jnp.float32),
                pltpu.VMEM((n_peer, rows, BN), jnp.float32),
                pltpu.VMEM((n_total, rows, BN), jnp.bfloat16),
                dma((2, KC)),
                dma((KC,)),
                dma((2,)),
                dma((2,)),
                dma((n_part,)),
                dma((n_peer,)),
                dma((n_total,)),
                dma((n_total,)),
                dma((blocks,)),
                dma((n_total,)),
                dma((blocks,)),
                dma((blocks,)),
                dma((blocks,)),
            ],
            compiler_params=pltpu.CompilerParams(
                collective_id=0, has_side_effects=True, vmem_limit_bytes=58 * 1024 * 1024
            ),
            cost_estimate=pl.CostEstimate(
                flops=4 * rows * width * cols,
                bytes_accessed=2 * width * cols,
                transcendentals=0,
            ),
        )(x_one, x_two, w_down)

    return jax.shard_map(
        per_device,
        mesh=mesh,
        in_specs=(P("data", "tp"), P("data", "tp"), P("tp", None)),
        out_specs=(P("data", None), P("data", None)),
        check_vma=False,
    )
```

```python
import jax
import jax.numpy as jnp
from jax import lax
from jax.experimental import pallas as pl
from jax.experimental.pallas import tpu as pltpu
from jax.sharding import PartitionSpec as P

MESH = pl.DeviceIdType.MESH
LEAD = 3
BN = 256
KC = 6
LATE = 8


def kernel(
    x_one, x_two, w, y_one, y_two, h_one, h_two,
    wbuf, acc, pair, part, own, peer, total,
    x_sem, w_sem, pair_send, pair_recv, part_send, part_recv,
    y_local, y_pair_send, y_pair_recv, y_send, y_recv, fwd_send, fwd_recv,
    back_sem, late_sem, free_sem,
):
    rows, width = x_one.shape
    cols = w.shape[1]
    kb = width // KC
    np_ = cols // BN // 2
    steps = 2 * np_
    big = 2 * steps
    n_part, n_peer, n_total = part.shape[0], peer.shape[0], total.shape[0]
    early = np_ - LATE

    t = lax.axis_index("tp")
    chip, lane = lax.div(t, 2), lax.rem(t, 2)
    sibling = {"tp": 2 * chip + 1 - lane}
    across = {"tp": 2 * (1 - chip) + lane}

    def at_least(s, a):
        return lax.div(s + big - a, big)

    def is_peer(s):
        head = 1 - at_least(s, LEAD)
        tail = at_least(s, steps - LEAD)
        return head + (1 - head - tail) * lax.rem(s + LEAD + 2, 2)

    def index(s):
        head = 1 - at_least(s, LEAD)
        tail = at_least(s, steps - LEAD)
        mid = 1 - head - tail
        odd = lax.rem(s + LEAD + 2, 2)
        u = s - LEAD + big
        return head * s + tail * (s - np_) + mid * (lax.div(u, 2) - big // 2 + odd * LEAD)

    def columns(owner, j, n=1):
        return pl.ds(pl.multiple_of((owner * np_ + j) * BN, BN), n * BN)

    def block_columns(s):
        p = is_peer(s)
        return columns(chip + p * (1 - 2 * chip), index(s))

    def w_copy(s, k):
        return pltpu.make_async_copy(
            w.at[pl.ds(k * kb, kb), block_columns(s)], wbuf.at[k], w_sem.at[k]
        )

    def x_copy(k, m):
        x, y = ((x_one, y_one), (x_two, y_two))[m]
        at = pl.ds(k * kb, kb)
        return pltpu.make_async_copy(x.at[:, at], y.at[:, at], x_sem.at[m, k])

    def x_rows(k, m, lo, n):
        return (y_one, y_two)[m][lo : lo + n, k * kb : (k + 1) * kb]

    def half(slot, which):
        return acc.at[slot, pl.ds(pl.multiple_of(which * rows, rows), rows)]

    def pair_copy(s):
        slot = lax.rem(s, 2)
        return pltpu.make_async_remote_copy(
            half(slot, 1 - lane), pair.at[slot], pair_send.at[slot], pair_recv.at[slot],
            device_id=sibling, device_id_type=MESH,
        )

    def part_copy(j):
        a, b = lax.rem(j, n_part), lax.rem(j, n_peer)
        return pltpu.make_async_remote_copy(
            part.at[a], peer.at[b], part_send.at[a], part_recv.at[b],
            device_id=across, device_id_type=MESH,
        )

    def y_across(y, j):
        a = lax.rem(j, n_total)
        return pltpu.make_async_remote_copy(
            total.at[a], y.at[:, columns(chip, j)], y_send.at[a], y_recv.at[j],
            device_id=across, device_id_type=MESH,
        )

    def y_pair(y, j):
        a = lax.rem(j, n_total)
        return pltpu.make_async_remote_copy(
            total.at[a], y.at[:, columns(chip, j)], y_pair_send.at[a], y_pair_recv.at[j],
            device_id=sibling, device_id_type=MESH,
        )

    def y_here(y, j):
        a = lax.rem(j, n_total)
        return pltpu.make_async_copy(total.at[a], y.at[:, columns(chip, j)], y_local.at[a])

    def fwd_copy(y, j):
        ref = y.at[:, columns(1 - chip, j)]
        return pltpu.make_async_remote_copy(
            ref, ref, fwd_send.at[j], fwd_recv.at[j], device_id=sibling, device_id_type=MESH
        )

    def back_copy(h, y, owner, j, n, sem):
        at = columns(owner, j, n)
        return pltpu.make_async_copy(h.at[:, at], y.at[:, at], sem)

    def by_lane(f, which=None):
        which = lane if which is None else which

        @pl.when(which == 0)
        def _():
            f(h_one, y_one)

        @pl.when(which == 1)
        def _():
            f(h_two, y_two)

    def add_pair(s):
        slot = lax.rem(s, 2)
        p, j = is_peer(s), index(s)
        pair_copy(s).wait_recv()

        @pl.when(p == 1)
        def _():
            @pl.when(j >= n_part)
            def _():
                part_copy(j - n_part).wait_send()

            part[lax.rem(j, n_part)] = half(slot, lane)[...] + pair[slot]
            part_copy(j).start()

        @pl.when(p == 0)
        def _():
            own[lax.rem(j, 2)] = half(slot, lane)[...] + pair[slot]

    def wait_total(j):
        y_across(h_one, j).wait_send()
        y_pair(h_one, j).wait_send()
        y_here(h_one, j).wait()

    def finish(j):
        part_copy(j).wait_recv()

        @pl.when(j >= n_total)
        def _():
            wait_total(j - n_total)

        total[lax.rem(j, n_total)] = (
            own[lax.rem(j, 2)] + peer[lax.rem(j, n_peer)]
        ).astype(jnp.bfloat16)

    def send_total(j):
        def send(h, y):
            y_across(h, j).start()
            y_pair(h, j).start()
            y_here(h, j).start()

        by_lane(send)

    def forward(j):
        y_across(h_one, j).wait_recv()
        by_lane(lambda h, y: fwd_copy(h, j).start())

    for k in range(KC):
        x_copy(k, 0).start()
        w_copy(0, k).start()

    barrier = pltpu.get_barrier_semaphore()
    for other in (sibling, across):
        pl.semaphore_signal(barrier, inc=1, device_id=other, device_id_type=MESH)
    pl.semaphore_wait(barrier, 2)

    quarter = rows // 2
    for m in range(2):
        for k in range(KC):
            x_copy(k, m).wait()
            if m == 0:
                w_copy(0, k).wait()
                if k >= KC // 2:
                    x_copy(2 * k - KC, 1).start()
                    x_copy(2 * k - KC + 1, 1).start()
            for q in range(2):
                at = pl.ds(m * rows + q * quarter, quarter)
                product = jnp.dot(
                    x_rows(k, m, q * quarter, quarter), wbuf[k],
                    preferred_element_type=jnp.float32,
                )
                if k == 0:
                    acc[0, at] = product
                else:
                    acc[0, at] += product
            if m == 1:
                w_copy(1, k).start()
                if k == 2:
                    @pl.when(lane == 0)
                    def _():
                        add_pair(0)

        @pl.when(lane == 1 - m)
        def _():
            pair_copy(0).start()

    def step(s, carry):
        slot = lax.rem(s, 2)
        before = jnp.maximum(s - 2, 0)

        def own_two_back(f):
            @pl.when(s >= 2)
            def _():
                @pl.when(is_peer(before) == 0)
                def _():
                    f(index(before))

        def forward_behind(j):
            @pl.when(j >= LEAD + 1)
            def _():
                forward(j - LEAD - 1)

        for k in range(KC):
            w_copy(s, k).wait()
            for m in range(2):
                at = pl.ds(m * rows, rows)
                product = jnp.dot(
                    x_rows(k, m, 0, rows), wbuf[k], preferred_element_type=jnp.float32
                )
                if k == 0:
                    acc[slot, at] = product
                else:
                    acc[slot, at] += product

            @pl.when(s + 1 < steps)
            def _():
                w_copy(s + 1, k).start()

            if k == 1:
                pair_copy(s - 1).wait_send()

                @pl.when(s + lane >= 2)
                def _():
                    add_pair(s - 1)
            if k == 2:
                own_two_back(finish)
            if k == 3:
                own_two_back(send_total)
            if k == 4:
                own_two_back(forward_behind)

        pair_copy(s).start()
        return carry

    lax.fori_loop(1, steps, step, 0)

    for other in (sibling, across):
        pl.semaphore_signal(free_sem, inc=1, device_id=other, device_id_type=MESH)

    def landed(j, carry):
        y_pair(h_one, j).wait_recv()
        fwd_copy(h_one, j).wait_recv()
        return carry

    lax.fori_loop(0, early, landed, 0)
    bulk = [
        back_copy(h, y, owner, 0, early, back_sem.at[m, owner])
        for m, (h, y) in enumerate(((h_one, y_one), (h_two, y_two)))
        for owner in range(2)
    ]
    for c in bulk:
        c.start()

    last = np_ - 1
    pair_copy(steps - 1).wait_send()
    add_pair(steps - 1)
    for j in range(np_ - 2 - LEAD - 1, last - LEAD):
        forward(j)
    finish(last - 1)
    send_total(last - 1)
    forward(last - LEAD - 1 + 1)
    finish(last)
    pl.semaphore_wait(free_sem, 2)

    def send_last(h, y):
        y_across(y, last).start()
        y_pair(y, last).start()
        y[:, columns(chip, last)] = total[last % n_total]

    by_lane(send_last)

    for j in range(np_ - n_total, last):
        y_here(h_one, j).wait()
    by_lane(lambda h, y: back_copy(h, y, chip, early, LATE - 1, late_sem.at[0]).start())
    for j in range(early, np_):
        y_pair(h_one, j).wait_recv()
    by_lane(
        lambda h, y: back_copy(h, y, chip, early, LATE - 1, late_sem.at[1]).start(), 1 - lane
    )

    for j in range(last - LEAD + 1, last):
        forward(j)
    by_lane(lambda h, y: back_copy(h, y, 1 - chip, early, LATE - 1, late_sem.at[2]).start())
    for j in range(early, last):
        fwd_copy(h_one, j).wait_recv()
    by_lane(
        lambda h, y: back_copy(h, y, 1 - chip, early, LATE - 1, late_sem.at[3]).start(), 1 - lane
    )
    y_across(y_one, last).wait_recv()
    by_lane(lambda h, y: fwd_copy(y, last).start())

    for c in bulk:
        c.wait()
    for a in range(4):
        back_copy(h_one, y_one, 0, early, LATE - 1, late_sem.at[a]).wait()
    for j in range(np_ - n_part, np_):
        part_copy(j).wait_send()
    for j in range(np_ - n_total, np_):
        y_across(h_one, j).wait_send()
        y_pair(h_one, j).wait_send()

    def sent(j, carry):
        fwd_copy(h_one, j).wait_send()
        return carry

    lax.fori_loop(0, np_, sent, 0)
    fwd_copy(y_one, last).wait_recv()


def solution(mesh):
    def per_device(x_one, x_two, w_down):
        rows, width = x_one.shape
        cols = w_down.shape[1]
        blocks = cols // BN // 2
        n_part, n_peer, n_total = LEAD + 2, 2 * LEAD + 2, LEAD + 2
        dma = pltpu.SemaphoreType.DMA
        out = jax.ShapeDtypeStruct((rows, cols), jnp.bfloat16)
        hbm = pl.BlockSpec(memory_space=pltpu.HBM)
        vmem = pl.BlockSpec(memory_space=pltpu.VMEM)
        return pl.pallas_call(
            kernel,
            out_shape=(out, out, out, out),
            in_specs=[hbm] * 3,
            out_specs=(vmem, vmem, hbm, hbm),
            scratch_shapes=[
                pltpu.VMEM((KC, width // KC, BN), jnp.bfloat16),
                pltpu.VMEM((2, 2 * rows, BN), jnp.float32),
                pltpu.VMEM((2, rows, BN), jnp.float32),
                pltpu.VMEM((n_part, rows, BN), jnp.float32),
                pltpu.VMEM((2, rows, BN), jnp.float32),
                pltpu.VMEM((n_peer, rows, BN), jnp.float32),
                pltpu.VMEM((n_total, rows, BN), jnp.bfloat16),
                dma((2, KC)),
                dma((KC,)),
                dma((2,)),
                dma((2,)),
                dma((n_part,)),
                dma((n_peer,)),
                dma((n_total,)),
                dma((n_total,)),
                dma((blocks,)),
                dma((n_total,)),
                dma((blocks,)),
                dma((blocks,)),
                dma((blocks,)),
                dma((2, 2)),
                dma((4,)),
                pltpu.SemaphoreType.REGULAR,
            ],
            compiler_params=pltpu.CompilerParams(
                collective_id=0, has_side_effects=True, vmem_limit_bytes=24 * 1024 * 1024
            ),
            cost_estimate=pl.CostEstimate(
                flops=4 * rows * width * cols,
                bytes_accessed=2 * width * cols,
                transcendentals=0,
            ),
        )(x_one, x_two, w_down)[:2]

    return jax.shard_map(
        per_device,
        mesh=mesh,
        in_specs=(P("data", "tp"), P("data", "tp"), P("tp", None)),
        out_specs=(P("data", None), P("data", None)),
        check_vma=False,
    )
```

```python
import jax
import jax.numpy as jnp
from jax import lax
from jax.experimental import pallas as pl
from jax.experimental.pallas import tpu as pltpu
from jax.sharding import PartitionSpec as P

MESH = pl.DeviceIdType.MESH
LEAD = 4
BN = 256
KC = 6
AHEAD = 4
PIECES = 8
LATE = 8


def kernel(
    x_one, x_two, w, y_one, y_two, h_one, h_two,
    wbuf, acc, pair, part, own, peer, total,
    x_sem, w_sem, pair_send, pair_recv, part_send, part_recv,
    y_local, y_pair_send, y_pair_recv, y_send, y_recv, fwd_send, fwd_recv,
    back_sem, late_sem, first_send, first_recv, free_sem,
):
    rows, width = x_one.shape
    cols = w.shape[1]
    kb = width // KC
    np_ = cols // BN // 2
    steps = 2 * np_
    big = 2 * steps
    n_part, n_peer, n_total = part.shape[0], peer.shape[0], total.shape[0]
    early = np_ - LATE
    quarter = rows // 2

    t = lax.axis_index("tp")
    chip, lane = lax.div(t, 2), lax.rem(t, 2)
    sibling = {"tp": 2 * chip + 1 - lane}
    across = {"tp": 2 * (1 - chip) + lane}

    def at_least(s, a):
        return lax.div(s + big - a, big)

    def is_peer(s):
        head = 1 - at_least(s, LEAD)
        tail = at_least(s, steps - LEAD)
        return head + (1 - head - tail) * lax.rem(s + LEAD + 2, 2)

    def index(s):
        head = 1 - at_least(s, LEAD)
        tail = at_least(s, steps - LEAD)
        mid = 1 - head - tail
        odd = lax.rem(s + LEAD + 2, 2)
        u = s - LEAD + big
        return head * s + tail * (s - np_) + mid * (lax.div(u, 2) - big // 2 + odd * LEAD)

    def columns(owner, j, n=1):
        return pl.ds(pl.multiple_of((owner * np_ + j) * BN, BN), n * BN)

    def block_columns(s):
        p = is_peer(s)
        return columns(chip + p * (1 - 2 * chip), index(s))

    def w_copy(s, k):
        return pltpu.make_async_copy(
            w.at[pl.ds(k * kb, kb), block_columns(s)], wbuf.at[k], w_sem.at[k]
        )

    def x_copy(k, m, q):
        x, y = ((x_one, y_one), (x_two, y_two))[m]
        at = pl.ds(q * quarter, quarter), pl.ds(k * kb, kb)
        return pltpu.make_async_copy(x.at[at], y.at[at], x_sem.at[m, q, k])

    def x_rows(k, m, lo, n):
        return (y_one, y_two)[m][lo : lo + n, k * kb : (k + 1) * kb]

    def half(slot, which):
        return acc.at[slot, pl.ds(pl.multiple_of(which * rows, rows), rows)]

    def pair_copy(s):
        slot = lax.rem(s, 2)
        return pltpu.make_async_remote_copy(
            half(slot, 1 - lane), pair.at[slot], pair_send.at[slot], pair_recv.at[slot],
            device_id=sibling, device_id_type=MESH,
        )

    def part_copy(j):
        a, b = lax.rem(j, n_part), lax.rem(j, n_peer)
        return pltpu.make_async_remote_copy(
            part.at[a], peer.at[b], part_send.at[a], part_recv.at[b],
            device_id=across, device_id_type=MESH,
        )

    def y_across(y, j):
        a = lax.rem(j, n_total)
        return pltpu.make_async_remote_copy(
            total.at[a], y.at[:, columns(chip, j)], y_send.at[a], y_recv.at[j],
            device_id=across, device_id_type=MESH,
        )

    def y_pair(y, j):
        a = lax.rem(j, n_total)
        return pltpu.make_async_remote_copy(
            total.at[a], y.at[:, columns(chip, j)], y_pair_send.at[a], y_pair_recv.at[j],
            device_id=sibling, device_id_type=MESH,
        )

    def y_here(y, j):
        a = lax.rem(j, n_total)
        return pltpu.make_async_copy(total.at[a], y.at[:, columns(chip, j)], y_local.at[a])

    def fwd_copy(y, j):
        ref = y.at[:, columns(1 - chip, j)]
        return pltpu.make_async_remote_copy(
            ref, ref, fwd_send.at[j], fwd_recv.at[j], device_id=sibling, device_id_type=MESH
        )

    def back_copy(h, y, owner, j, n, sem):
        at = columns(owner, j, n)
        return pltpu.make_async_copy(h.at[:, at], y.at[:, at], sem)

    def by_lane(f, which=None):
        which = lane if which is None else which

        @pl.when(which == 0)
        def _():
            f(h_one, y_one)

        @pl.when(which == 1)
        def _():
            f(h_two, y_two)

    def add_pair(s):
        slot = lax.rem(s, 2)
        p, j = is_peer(s), index(s)
        pair_copy(s).wait_recv()

        @pl.when(p == 1)
        def _():
            @pl.when(j >= n_part)
            def _():
                part_copy(j - n_part).wait_send()

            part[lax.rem(j, n_part)] = half(slot, lane)[...] + pair[slot]
            part_copy(j).start()

        @pl.when(p == 0)
        def _():
            own[lax.rem(j, 2)] = half(slot, lane)[...] + pair[slot]

    def wait_total(j):
        y_across(h_one, j).wait_send()
        y_pair(h_one, j).wait_send()
        y_here(h_one, j).wait()

    def finish(j):
        part_copy(j).wait_recv()

        @pl.when(j >= n_total)
        def _():
            wait_total(j - n_total)

        total[lax.rem(j, n_total)] = (
            own[lax.rem(j, 2)] + peer[lax.rem(j, n_peer)]
        ).astype(jnp.bfloat16)

    def send_total(j):
        def send(h, y):
            y_across(h, j).start()
            y_pair(h, j).start()
            y_here(h, j).start()

        by_lane(send)

    def forward(j):
        y_across(h_one, j).wait_recv()
        by_lane(lambda h, y: fwd_copy(h, j).start())

    pieces = [(0, m, q * quarter, quarter) for m in range(2) for q in range(2)]
    pieces += [(1, m, 0, rows) for m in range(2)]

    def piece_copy(s, m, lo, n):
        q = lo // quarter
        send, recv = (first_send.at[q], first_recv.at[q]) if s == 0 else (
            pair_send.at[1], pair_recv.at[1])
        return pltpu.make_async_remote_copy(
            acc.at[s, pl.ds(m * rows + lo, n)], pair.at[s, pl.ds(lo, n)], send, recv,
            device_id=sibling, device_id_type=MESH,
        )

    def add_piece(s, m, lo, n):
        @pl.when(lane == m)
        def _():
            at = pl.ds(lo, n)
            piece_copy(s, m, lo, n).wait_recv()
            part[s, at] = acc[s, pl.ds(m * rows + lo, n)] + pair[s, at]
            pltpu.make_async_remote_copy(
                part.at[s, at], peer.at[s, at], part_send.at[s], part_recv.at[s],
                device_id=across, device_id_type=MESH,
            ).start()

    loads = [(x_copy(k, 0, 0), w_copy(0, k)) for k in range(KC)]
    loads += [(x_copy(k, m, q),) for m, q in ((0, 1), (1, 0), (1, 1)) for k in range(KC)]
    loads += [(w_copy(1, k),) for k in range(KC)]
    for load in loads[:AHEAD]:
        for c in load:
            c.start()

    barrier = pltpu.get_barrier_semaphore()
    for other in (sibling, across):
        pl.semaphore_signal(barrier, inc=1, device_id=other, device_id_type=MESH)
    pl.semaphore_wait(barrier, 2)

    for i, (s, m, lo, n) in enumerate(pieces):
        for k in range(KC):
            now = i * KC + k
            for c in loads[now] if now < len(loads) else ():
                c.wait()
            for c in loads[now + AHEAD] if now + AHEAD < len(loads) else ():
                c.start()
            for d in range(2):
                at = pl.ds(m * rows + lo + d * n // 2, n // 2)
                product = jnp.dot(
                    x_rows(k, m, lo + d * n // 2, n // 2), wbuf[k],
                    preferred_element_type=jnp.float32,
                )
                if k == 0:
                    acc[s, at] = product
                else:
                    acc[s, at] += product
            if i == len(pieces) - 1:
                w_copy(2, k).start()
            if i > 0 and k == (4 if n == quarter else 2):
                add_piece(*pieces[i - 1])

        @pl.when(lane == 1 - m)
        def _():
            piece_copy(s, m, lo, n).start()

    for q in range(2):
        piece_copy(0, 0, q * quarter, quarter).wait_send()

    def step(s, carry):
        slot = lax.rem(s, 2)

        def own_two_back(f):
            @pl.when(is_peer(s - 2) == 0)
            def _():
                f(index(s - 2))

        def forward_behind(j):
            @pl.when(j >= LEAD + 1)
            def _():
                forward(j - LEAD - 1)

        for k in range(KC):
            w_copy(s, k).wait()
            for m in range(2):
                at = pl.ds(m * rows, rows)
                product = jnp.dot(
                    x_rows(k, m, 0, rows), wbuf[k], preferred_element_type=jnp.float32
                )
                if k == 0:
                    acc[slot, at] = product
                else:
                    acc[slot, at] += product

            @pl.when(s + 1 < steps)
            def _():
                w_copy(s + 1, k).start()

            if k == 1:
                pair_copy(s - 1).wait_send()

                @pl.when(s + lane >= 3)
                def _():
                    add_pair(s - 1)
            if k == 2:
                own_two_back(finish)
            if k == 3:
                own_two_back(send_total)
            if k == 4:
                own_two_back(forward_behind)

        pair_copy(s).start()
        return carry

    lax.fori_loop(2, steps, step, 0)

    for other in (sibling, across):
        pl.semaphore_signal(free_sem, inc=1, device_id=other, device_id_type=MESH)

    def landed(j, carry):
        y_pair(h_one, j).wait_recv()
        fwd_copy(h_one, j).wait_recv()
        return carry

    lax.fori_loop(0, early, landed, 0)
    bulk = [
        back_copy(h, y, owner, 0, early, back_sem.at[m, owner])
        for m, (h, y) in enumerate(((h_one, y_one), (h_two, y_two)))
        for owner in range(2)
    ]
    for c in bulk:
        c.start()

    last = np_ - 1
    pair_copy(steps - 1).wait_send()
    add_pair(steps - 1)
    for j in range(np_ - 2 - LEAD - 1, last - LEAD):
        forward(j)
    finish(last - 1)
    send_total(last - 1)
    forward(last - LEAD - 1 + 1)
    finish(last)
    pl.semaphore_wait(free_sem, 2)

    def send_last(h, y):
        y_across(y, last).start()
        y_pair(y, last).start()
        y[:, columns(chip, last)] = total[last % n_total]

    by_lane(send_last)

    for j in range(np_ - n_total, last):
        y_here(h_one, j).wait()
    by_lane(lambda h, y: back_copy(h, y, chip, early, LATE - 1, late_sem.at[0]).start())
    for j in range(early, np_):
        y_pair(h_one, j).wait_recv()
    by_lane(
        lambda h, y: back_copy(h, y, chip, early, LATE - 1, late_sem.at[1]).start(), 1 - lane
    )

    for j in range(last - LEAD + 1, last):
        forward(j)
    by_lane(lambda h, y: back_copy(h, y, 1 - chip, early, LATE - 1, late_sem.at[2]).start())
    for j in range(early, last):
        fwd_copy(h_one, j).wait_recv()
    by_lane(
        lambda h, y: back_copy(h, y, 1 - chip, early, LATE - 1, late_sem.at[3]).start(), 1 - lane
    )
    y_across(y_one, last).wait_recv()
    by_lane(lambda h, y: fwd_copy(y, last).start())

    for c in bulk:
        c.wait()
    for a in range(4):
        back_copy(h_one, y_one, 0, early, LATE - 1, late_sem.at[a]).wait()
    for j in range(np_ - n_part, np_):
        part_copy(j).wait_send()
    for j in range(np_ - n_total, np_):
        y_across(h_one, j).wait_send()
        y_pair(h_one, j).wait_send()

    def sent(j, carry):
        fwd_copy(h_one, j).wait_send()
        return carry

    lax.fori_loop(0, np_, sent, 0)
    fwd_copy(y_one, last).wait_recv()


def to_result(a, b, y_one, y_two, sem):
    rows = a.shape[0] // PIECES
    copies = [
        pltpu.make_async_copy(
            src.at[pl.ds(i * rows, rows)], dst.at[pl.ds(i * rows, rows)], sem.at[m, i]
        )
        for i in range(PIECES)
        for m, (src, dst) in enumerate(((a, y_one), (b, y_two)))
    ]
    for c in copies:
        c.start()
    for c in copies:
        c.wait()


def solution(mesh):
    def per_device(x_one, x_two, w_down):
        rows, width = x_one.shape
        cols = w_down.shape[1]
        blocks = cols // BN // 2
        n_part, n_peer, n_total = LEAD + 2, 2 * LEAD + 2, LEAD + 2
        dma = pltpu.SemaphoreType.DMA
        out = jax.ShapeDtypeStruct((rows, cols), jnp.bfloat16)
        hbm = pl.BlockSpec(memory_space=pltpu.HBM)
        vmem = pl.BlockSpec(memory_space=pltpu.VMEM)
        y_one, y_two = pl.pallas_call(
            kernel,
            out_shape=(out, out, out, out),
            in_specs=[hbm] * 3,
            out_specs=(vmem, vmem, hbm, hbm),
            scratch_shapes=[
                pltpu.VMEM((KC, width // KC, BN), jnp.bfloat16),
                pltpu.VMEM((2, 2 * rows, BN), jnp.float32),
                pltpu.VMEM((2, rows, BN), jnp.float32),
                pltpu.VMEM((n_part, rows, BN), jnp.float32),
                pltpu.VMEM((2, rows, BN), jnp.float32),
                pltpu.VMEM((n_peer, rows, BN), jnp.float32),
                pltpu.VMEM((n_total, rows, BN), jnp.bfloat16),
                dma((2, 2, KC)),
                dma((KC,)),
                dma((2,)),
                dma((2,)),
                dma((n_part,)),
                dma((n_peer,)),
                dma((n_total,)),
                dma((n_total,)),
                dma((blocks,)),
                dma((n_total,)),
                dma((blocks,)),
                dma((blocks,)),
                dma((blocks,)),
                dma((2, 2)),
                dma((4,)),
                dma((2,)),
                dma((2,)),
                pltpu.SemaphoreType.REGULAR,
            ],
            compiler_params=pltpu.CompilerParams(
                collective_id=0, has_side_effects=True, vmem_limit_bytes=24 * 1024 * 1024
            ),
            cost_estimate=pl.CostEstimate(
                flops=4 * rows * width * cols,
                bytes_accessed=2 * width * cols,
                transcendentals=0,
            ),
        )(x_one, x_two, w_down)[:2]
        return pl.pallas_call(
            to_result,
            out_shape=(out, out),
            in_specs=[vmem] * 2,
            out_specs=(hbm, hbm),
            scratch_shapes=[dma((2, PIECES))],
            compiler_params=pltpu.CompilerParams(vmem_limit_bytes=1024 * 1024),
            cost_estimate=pl.CostEstimate(
                flops=0, bytes_accessed=8 * rows * cols, transcendentals=0
            ),
        )(y_one, y_two)

    return jax.shard_map(
        per_device,
        mesh=mesh,
        in_specs=(P("data", "tp"), P("data", "tp"), P("tp", None)),
        out_specs=(P("data", None), P("data", None)),
        check_vma=False,
    )
```

```python
import jax
import jax.numpy as jnp
from jax import lax
from jax.experimental import pallas as pl
from jax.experimental.pallas import tpu as pltpu
from jax.sharding import PartitionSpec as P

MESH = pl.DeviceIdType.MESH
LEAD = 4
BN = 256
KC = 6
AHEAD = 4
PIECES = 8
LAST = 4
LATE = 8


def kernel(
    x_one, x_two, w, y_one, y_two, h_one, h_two,
    wbuf, acc, pair, part, own, peer, total,
    x_sem, w_sem, pair_send, pair_recv, part_send, part_recv,
    y_local, y_pair_send, y_pair_recv, y_send, y_recv, fwd_send, fwd_recv,
    back_sem, late_sem, first_send, first_recv, last_recv, free_sem,
):
    rows, width = x_one.shape
    cols = w.shape[1]
    kb = width // KC
    np_ = cols // BN // 2
    steps = 2 * np_
    big = 2 * steps
    n_part, n_peer, n_total = part.shape[0], peer.shape[0], total.shape[0]
    early = np_ - LATE
    quarter = rows // 2

    t = lax.axis_index("tp")
    chip, lane = lax.div(t, 2), lax.rem(t, 2)
    sibling = {"tp": 2 * chip + 1 - lane}
    across = {"tp": 2 * (1 - chip) + lane}

    def at_least(s, a):
        return lax.div(s + big - a, big)

    def is_peer(s):
        head = 1 - at_least(s, LEAD)
        tail = at_least(s, steps - LEAD)
        return head + (1 - head - tail) * lax.rem(s + LEAD + 2, 2)

    def index(s):
        head = 1 - at_least(s, LEAD)
        tail = at_least(s, steps - LEAD)
        mid = 1 - head - tail
        odd = lax.rem(s + LEAD + 2, 2)
        u = s - LEAD + big
        return head * s + tail * (s - np_) + mid * (lax.div(u, 2) - big // 2 + odd * LEAD)

    def columns(owner, j, n=1):
        return pl.ds(pl.multiple_of((owner * np_ + j) * BN, BN), n * BN)

    def block_columns(s):
        p = is_peer(s)
        return columns(chip + p * (1 - 2 * chip), index(s))

    def w_copy(s, k):
        return pltpu.make_async_copy(
            w.at[pl.ds(k * kb, kb), block_columns(s)], wbuf.at[k], w_sem.at[k]
        )

    def x_copy(k, m, q):
        x, y = ((x_one, y_one), (x_two, y_two))[m]
        at = pl.ds(q * quarter, quarter), pl.ds(k * kb, kb)
        return pltpu.make_async_copy(x.at[at], y.at[at], x_sem.at[m, q, k])

    def x_rows(k, m, lo, n):
        return (y_one, y_two)[m][lo : lo + n, k * kb : (k + 1) * kb]

    def half(slot, which):
        return acc.at[slot, pl.ds(pl.multiple_of(which * rows, rows), rows)]

    def pair_copy(s):
        slot = lax.rem(s, 2)
        return pltpu.make_async_remote_copy(
            half(slot, 1 - lane), pair.at[slot], pair_send.at[slot], pair_recv.at[slot],
            device_id=sibling, device_id_type=MESH,
        )

    def part_copy(j):
        a, b = lax.rem(j, n_part), lax.rem(j, n_peer)
        return pltpu.make_async_remote_copy(
            part.at[a], peer.at[b], part_send.at[a], part_recv.at[b],
            device_id=across, device_id_type=MESH,
        )

    def y_across(y, j):
        a = lax.rem(j, n_total)
        return pltpu.make_async_remote_copy(
            total.at[a], y.at[:, columns(chip, j)], y_send.at[a], y_recv.at[j],
            device_id=across, device_id_type=MESH,
        )

    def y_pair(y, j):
        a = lax.rem(j, n_total)
        return pltpu.make_async_remote_copy(
            total.at[a], y.at[:, columns(chip, j)], y_pair_send.at[a], y_pair_recv.at[j],
            device_id=sibling, device_id_type=MESH,
        )

    def y_here(y, j):
        a = lax.rem(j, n_total)
        return pltpu.make_async_copy(total.at[a], y.at[:, columns(chip, j)], y_local.at[a])

    def fwd_copy(y, j):
        ref = y.at[:, columns(1 - chip, j)]
        return pltpu.make_async_remote_copy(
            ref, ref, fwd_send.at[j], fwd_recv.at[j], device_id=sibling, device_id_type=MESH
        )

    def back_copy(h, y, owner, j, n, sem):
        at = columns(owner, j, n)
        return pltpu.make_async_copy(h.at[:, at], y.at[:, at], sem)

    def by_lane(f, which=None):
        which = lane if which is None else which

        @pl.when(which == 0)
        def _():
            f(h_one, y_one)

        @pl.when(which == 1)
        def _():
            f(h_two, y_two)

    def add_pair(s):
        slot = lax.rem(s, 2)
        p, j = is_peer(s), index(s)
        pair_copy(s).wait_recv()

        @pl.when(p == 1)
        def _():
            @pl.when(j >= n_part)
            def _():
                part_copy(j - n_part).wait_send()

            part[lax.rem(j, n_part)] = half(slot, lane)[...] + pair[slot]
            part_copy(j).start()

        @pl.when(p == 0)
        def _():
            own[lax.rem(j, 2)] = half(slot, lane)[...] + pair[slot]

    def wait_total(j):
        y_across(h_one, j).wait_send()
        y_pair(h_one, j).wait_send()
        y_here(h_one, j).wait()

    def finish(j):
        part_copy(j).wait_recv()

        @pl.when(j >= n_total)
        def _():
            wait_total(j - n_total)

        total[lax.rem(j, n_total)] = (
            own[lax.rem(j, 2)] + peer[lax.rem(j, n_peer)]
        ).astype(jnp.bfloat16)

    def send_total(j):
        def send(h, y):
            y_across(h, j).start()
            y_pair(h, j).start()
            y_here(h, j).start()

        by_lane(send)

    def forward(j):
        y_across(h_one, j).wait_recv()
        by_lane(lambda h, y: fwd_copy(h, j).start())

    pieces = [(0, m, q * quarter, quarter) for m in range(2) for q in range(2)]
    pieces += [(1, m, 0, rows) for m in range(2)]

    def piece_copy(s, m, lo, n):
        q = lo // quarter
        send, recv = (first_send.at[q], first_recv.at[q]) if s == 0 else (
            pair_send.at[1], pair_recv.at[1])
        return pltpu.make_async_remote_copy(
            acc.at[s, pl.ds(m * rows + lo, n)], pair.at[s, pl.ds(lo, n)], send, recv,
            device_id=sibling, device_id_type=MESH,
        )

    def add_piece(s, m, lo, n):
        @pl.when(lane == m)
        def _():
            at = pl.ds(lo, n)
            piece_copy(s, m, lo, n).wait_recv()
            part[s, at] = acc[s, pl.ds(m * rows + lo, n)] + pair[s, at]
            pltpu.make_async_remote_copy(
                part.at[s, at], peer.at[s, at], part_send.at[s], part_recv.at[s],
                device_id=across, device_id_type=MESH,
            ).start()

    loads = [(x_copy(k, 0, 0), w_copy(0, k)) for k in range(KC)]
    loads += [(x_copy(k, m, q),) for m, q in ((0, 1), (1, 0), (1, 1)) for k in range(KC)]
    loads += [(w_copy(1, k),) for k in range(KC)]
    for load in loads[:AHEAD]:
        for c in load:
            c.start()

    barrier = pltpu.get_barrier_semaphore()
    for other in (sibling, across):
        pl.semaphore_signal(barrier, inc=1, device_id=other, device_id_type=MESH)

    for i, (s, m, lo, n) in enumerate(pieces):
        for k in range(KC):
            now = i * KC + k
            for c in loads[now] if now < len(loads) else ():
                c.wait()
            for c in loads[now + AHEAD] if now + AHEAD < len(loads) else ():
                c.start()
            for d in range(2):
                at = pl.ds(m * rows + lo + d * n // 2, n // 2)
                product = jnp.dot(
                    x_rows(k, m, lo + d * n // 2, n // 2), wbuf[k],
                    preferred_element_type=jnp.float32,
                )
                if k == 0:
                    acc[s, at] = product
                else:
                    acc[s, at] += product
            if i == len(pieces) - 1:
                w_copy(2, k).start()
            if i > 0 and k == (4 if n == quarter else 2):
                add_piece(*pieces[i - 1])

        if i == 0:
            pl.semaphore_wait(barrier, 2)

        @pl.when(lane == 1 - m)
        def _():
            piece_copy(s, m, lo, n).start()

    for q in range(2):
        piece_copy(0, 0, q * quarter, quarter).wait_send()

    def step(s, carry):
        slot = lax.rem(s, 2)

        def own_two_back(f):
            @pl.when(is_peer(s - 2) == 0)
            def _():
                f(index(s - 2))

        def forward_behind(j):
            @pl.when(j >= LEAD + 1)
            def _():
                forward(j - LEAD - 1)

        for k in range(KC):
            w_copy(s, k).wait()
            for m in range(2):
                at = pl.ds(m * rows, rows)
                product = jnp.dot(
                    x_rows(k, m, 0, rows), wbuf[k], preferred_element_type=jnp.float32
                )
                if k == 0:
                    acc[slot, at] = product
                else:
                    acc[slot, at] += product

            @pl.when(s + 1 < steps)
            def _():
                w_copy(s + 1, k).start()

            if k == 1:
                pair_copy(s - 1).wait_send()

                @pl.when(s + lane >= 3)
                def _():
                    add_pair(s - 1)
            if k == 2:
                own_two_back(finish)
            if k == 3:
                own_two_back(send_total)
            if k == 4:
                own_two_back(forward_behind)

        pair_copy(s).start()
        return carry

    lax.fori_loop(2, steps, step, 0)

    for other in (sibling, across):
        pl.semaphore_signal(free_sem, inc=1, device_id=other, device_id_type=MESH)

    def landed(j, carry):
        y_pair(h_one, j).wait_recv()
        fwd_copy(h_one, j).wait_recv()
        return carry

    lax.fori_loop(0, early, landed, 0)
    bulk = [
        back_copy(h, y, owner, 0, early, back_sem.at[m, owner])
        for m, (h, y) in enumerate(((h_one, y_one), (h_two, y_two)))
        for owner in range(2)
    ]
    for c in bulk:
        c.start()

    last = np_ - 1
    pair_copy(steps - 1).wait_send()
    add_pair(steps - 1)
    for j in range(np_ - 2 - LEAD - 1, last - LEAD):
        forward(j)
    finish(last - 1)
    send_total(last - 1)
    forward(last - LEAD - 1 + 1)
    finish(last)
    pl.semaphore_wait(free_sem, 2)

    cut = rows // LAST

    def last_across(y, i):
        at = pl.ds(i * cut, cut)
        return pltpu.make_async_remote_copy(
            total.at[last % n_total, at], y.at[at, columns(chip, last)],
            y_send.at[last % n_total], last_recv.at[i],
            device_id=across, device_id_type=MESH,
        )

    def last_fwd(y, i):
        ref = y.at[pl.ds(i * cut, cut), columns(1 - chip, last)]
        return pltpu.make_async_remote_copy(
            ref, ref, fwd_send.at[last], fwd_recv.at[last],
            device_id=sibling, device_id_type=MESH,
        )

    def send_last(h, y):
        for i in range(LAST):
            last_across(y, i).start()
        y_pair(y, last).start()
        y[:, columns(chip, last)] = total[last % n_total]

    by_lane(send_last)

    for j in range(np_ - n_total, last):
        y_here(h_one, j).wait()
    by_lane(lambda h, y: back_copy(h, y, chip, early, LATE - 1, late_sem.at[0]).start())
    for j in range(early, np_):
        y_pair(h_one, j).wait_recv()
    by_lane(
        lambda h, y: back_copy(h, y, chip, early, LATE - 1, late_sem.at[1]).start(), 1 - lane
    )

    for j in range(last - LEAD + 1, last):
        forward(j)
    by_lane(lambda h, y: back_copy(h, y, 1 - chip, early, LATE - 1, late_sem.at[2]).start())
    for j in range(early, last):
        fwd_copy(h_one, j).wait_recv()
    by_lane(
        lambda h, y: back_copy(h, y, 1 - chip, early, LATE - 1, late_sem.at[3]).start(), 1 - lane
    )
    for i in range(LAST):
        last_across(y_one, i).wait_recv()
        by_lane(lambda h, y: last_fwd(y, i).start())

    for c in bulk:
        c.wait()
    for a in range(4):
        back_copy(h_one, y_one, 0, early, LATE - 1, late_sem.at[a]).wait()
    for j in range(np_ - n_part, np_):
        part_copy(j).wait_send()
    for j in range(np_ - n_total, np_):
        y_across(h_one, j).wait_send()
        y_pair(h_one, j).wait_send()

    def sent(j, carry):
        fwd_copy(h_one, j).wait_send()
        return carry

    lax.fori_loop(0, np_, sent, 0)
    fwd_copy(y_one, last).wait_recv()


def to_result(a, b, y_one, y_two, sem):
    rows = a.shape[0] // PIECES
    copies = [
        pltpu.make_async_copy(
            src.at[pl.ds(i * rows, rows)], dst.at[pl.ds(i * rows, rows)], sem.at[m, i]
        )
        for i in range(PIECES)
        for m, (src, dst) in enumerate(((a, y_one), (b, y_two)))
    ]
    for c in copies:
        c.start()
    for c in copies:
        c.wait()


def solution(mesh):
    def per_device(x_one, x_two, w_down):
        rows, width = x_one.shape
        cols = w_down.shape[1]
        blocks = cols // BN // 2
        n_part, n_peer, n_total = LEAD + 2, 2 * LEAD + 2, LEAD + 2
        dma = pltpu.SemaphoreType.DMA
        out = jax.ShapeDtypeStruct((rows, cols), jnp.bfloat16)
        hbm = pl.BlockSpec(memory_space=pltpu.HBM)
        vmem = pl.BlockSpec(memory_space=pltpu.VMEM)
        y_one, y_two = pl.pallas_call(
            kernel,
            out_shape=(out, out, out, out),
            in_specs=[hbm] * 3,
            out_specs=(vmem, vmem, hbm, hbm),
            scratch_shapes=[
                pltpu.VMEM((KC, width // KC, BN), jnp.bfloat16),
                pltpu.VMEM((2, 2 * rows, BN), jnp.float32),
                pltpu.VMEM((2, rows, BN), jnp.float32),
                pltpu.VMEM((n_part, rows, BN), jnp.float32),
                pltpu.VMEM((2, rows, BN), jnp.float32),
                pltpu.VMEM((n_peer, rows, BN), jnp.float32),
                pltpu.VMEM((n_total, rows, BN), jnp.bfloat16),
                dma((2, 2, KC)),
                dma((KC,)),
                dma((2,)),
                dma((2,)),
                dma((n_part,)),
                dma((n_peer,)),
                dma((n_total,)),
                dma((n_total,)),
                dma((blocks,)),
                dma((n_total,)),
                dma((blocks,)),
                dma((blocks,)),
                dma((blocks,)),
                dma((2, 2)),
                dma((4,)),
                dma((2,)),
                dma((2,)),
                dma((LAST,)),
                pltpu.SemaphoreType.REGULAR,
            ],
            compiler_params=pltpu.CompilerParams(
                collective_id=0, has_side_effects=True, vmem_limit_bytes=24 * 1024 * 1024
            ),
            cost_estimate=pl.CostEstimate(
                flops=4 * rows * width * cols,
                bytes_accessed=2 * width * cols,
                transcendentals=0,
            ),
        )(x_one, x_two, w_down)[:2]
        return pl.pallas_call(
            to_result,
            out_shape=(out, out),
            in_specs=[vmem] * 2,
            out_specs=(hbm, hbm),
            scratch_shapes=[dma((2, PIECES))],
            compiler_params=pltpu.CompilerParams(vmem_limit_bytes=1024 * 1024),
            cost_estimate=pl.CostEstimate(
                flops=0, bytes_accessed=8 * rows * cols, transcendentals=0
            ),
        )(y_one, y_two)

    return jax.shard_map(
        per_device,
        mesh=mesh,
        in_specs=(P("data", "tp"), P("data", "tp"), P("tp", None)),
        out_specs=(P("data", None), P("data", None)),
        check_vma=False,
    )
```

```python
import jax
import jax.numpy as jnp
from jax import lax
from jax.experimental import pallas as pl
from jax.experimental.pallas import tpu as pltpu
from jax.sharding import PartitionSpec as P

MESH = pl.DeviceIdType.MESH
LEAD = 4
BN = 256
KC = 6
AHEAD = 5
PIECES = 4
LAST = 4
LATE = 8


def kernel(
    x_one, x_two, w, y_one, y_two, h_one, h_two,
    wbuf, acc, pair, part, own, peer, total,
    x_sem, w_sem, pair_send, pair_recv, part_send, part_recv,
    y_local, y_pair_send, y_pair_recv, y_send, y_recv, fwd_send, fwd_recv,
    back_sem, late_sem, first_send, first_recv, last_recv, free_sem,
):
    rows, width = x_one.shape
    cols = w.shape[1]
    kb = width // KC
    np_ = cols // BN // 2
    steps = 2 * np_
    big = 2 * steps
    n_part, n_peer, n_total = part.shape[0], peer.shape[0], total.shape[0]
    early = np_ - LATE
    quarter = rows // 2

    t = lax.axis_index("tp")
    chip, lane = lax.div(t, 2), lax.rem(t, 2)
    sibling = {"tp": 2 * chip + 1 - lane}
    across = {"tp": 2 * (1 - chip) + lane}

    def at_least(s, a):
        return lax.div(s + big - a, big)

    def is_peer(s):
        head = 1 - at_least(s, LEAD)
        tail = at_least(s, steps - LEAD)
        return head + (1 - head - tail) * lax.rem(s + LEAD + 2, 2)

    def index(s):
        head = 1 - at_least(s, LEAD)
        tail = at_least(s, steps - LEAD)
        mid = 1 - head - tail
        odd = lax.rem(s + LEAD + 2, 2)
        u = s - LEAD + big
        return head * s + tail * (s - np_) + mid * (lax.div(u, 2) - big // 2 + odd * LEAD)

    def columns(owner, j, n=1):
        return pl.ds(pl.multiple_of((owner * np_ + j) * BN, BN), n * BN)

    def block_columns(s):
        p = is_peer(s)
        return columns(chip + p * (1 - 2 * chip), index(s))

    def w_copy(s, k):
        return pltpu.make_async_copy(
            w.at[pl.ds(k * kb, kb), block_columns(s)], wbuf.at[k], w_sem.at[k]
        )

    def x_copy(k, m, q):
        x, y = ((x_one, y_one), (x_two, y_two))[m]
        at = pl.ds(q * quarter, quarter), pl.ds(k * kb, kb)
        return pltpu.make_async_copy(x.at[at], y.at[at], x_sem.at[m, q, k])

    def x_rows(k, m, lo, n):
        return (y_one, y_two)[m][lo : lo + n, k * kb : (k + 1) * kb]

    def half(slot, which):
        return acc.at[slot, pl.ds(pl.multiple_of(which * rows, rows), rows)]

    def pair_copy(s):
        slot = lax.rem(s, 2)
        return pltpu.make_async_remote_copy(
            half(slot, 1 - lane), pair.at[slot], pair_send.at[slot], pair_recv.at[slot],
            device_id=sibling, device_id_type=MESH,
        )

    def part_copy(j):
        a, b = lax.rem(j, n_part), lax.rem(j, n_peer)
        return pltpu.make_async_remote_copy(
            part.at[a], peer.at[b], part_send.at[a], part_recv.at[b],
            device_id=across, device_id_type=MESH,
        )

    def y_across(y, j):
        a = lax.rem(j, n_total)
        return pltpu.make_async_remote_copy(
            total.at[a], y.at[:, columns(chip, j)], y_send.at[a], y_recv.at[j],
            device_id=across, device_id_type=MESH,
        )

    def y_pair(y, j):
        a = lax.rem(j, n_total)
        return pltpu.make_async_remote_copy(
            total.at[a], y.at[:, columns(chip, j)], y_pair_send.at[a], y_pair_recv.at[j],
            device_id=sibling, device_id_type=MESH,
        )

    def y_here(y, j):
        a = lax.rem(j, n_total)
        return pltpu.make_async_copy(total.at[a], y.at[:, columns(chip, j)], y_local.at[a])

    def fwd_copy(y, j):
        ref = y.at[:, columns(1 - chip, j)]
        return pltpu.make_async_remote_copy(
            ref, ref, fwd_send.at[j], fwd_recv.at[j], device_id=sibling, device_id_type=MESH
        )

    def back_copy(h, y, owner, j, n, sem):
        at = columns(owner, j, n)
        return pltpu.make_async_copy(h.at[:, at], y.at[:, at], sem)

    def by_lane(f, which=None):
        which = lane if which is None else which

        @pl.when(which == 0)
        def _():
            f(h_one, y_one)

        @pl.when(which == 1)
        def _():
            f(h_two, y_two)

    def add_pair(s):
        slot = lax.rem(s, 2)
        p, j = is_peer(s), index(s)
        pair_copy(s).wait_recv()

        @pl.when(p == 1)
        def _():
            @pl.when(j >= n_part)
            def _():
                part_copy(j - n_part).wait_send()

            part[lax.rem(j, n_part)] = half(slot, lane)[...] + pair[slot]
            part_copy(j).start()

        @pl.when(p == 0)
        def _():
            own[lax.rem(j, 2)] = half(slot, lane)[...] + pair[slot]

    def wait_total(j):
        y_across(h_one, j).wait_send()
        y_pair(h_one, j).wait_send()
        y_here(h_one, j).wait()

    def finish(j):
        part_copy(j).wait_recv()

        @pl.when(j >= n_total)
        def _():
            wait_total(j - n_total)

        total[lax.rem(j, n_total)] = (
            own[lax.rem(j, 2)] + peer[lax.rem(j, n_peer)]
        ).astype(jnp.bfloat16)

    def send_total(j):
        def send(h, y):
            y_across(h, j).start()
            y_pair(h, j).start()
            y_here(h, j).start()

        by_lane(send)

    def forward(j):
        y_across(h_one, j).wait_recv()
        by_lane(lambda h, y: fwd_copy(h, j).start())

    pieces = [(0, m, q * quarter, quarter) for m in range(2) for q in range(2)]
    pieces += [(1, m, 0, rows) for m in range(2)]

    def piece_copy(s, m, lo, n):
        q = lo // quarter
        send, recv = (first_send.at[q], first_recv.at[q]) if s == 0 else (
            pair_send.at[1], pair_recv.at[1])
        return pltpu.make_async_remote_copy(
            acc.at[s, pl.ds(m * rows + lo, n)], pair.at[s, pl.ds(lo, n)], send, recv,
            device_id=sibling, device_id_type=MESH,
        )

    def add_piece(s, m, lo, n):
        @pl.when(lane == m)
        def _():
            at = pl.ds(lo, n)
            piece_copy(s, m, lo, n).wait_recv()
            part[s, at] = acc[s, pl.ds(m * rows + lo, n)] + pair[s, at]
            pltpu.make_async_remote_copy(
                part.at[s, at], peer.at[s, at], part_send.at[s], part_recv.at[s],
                device_id=across, device_id_type=MESH,
            ).start()

    loads = [(x_copy(k, 0, 0), w_copy(0, k)) for k in range(KC)]
    loads += [(x_copy(k, m, q),) for m, q in ((0, 1), (1, 0), (1, 1)) for k in range(KC)]
    loads += [(w_copy(1, k),) for k in range(KC)]
    for load in loads[:AHEAD]:
        for c in load:
            c.start()

    barrier = pltpu.get_barrier_semaphore()
    for other in (sibling, across):
        pl.semaphore_signal(barrier, inc=1, device_id=other, device_id_type=MESH)

    for i, (s, m, lo, n) in enumerate(pieces):
        for k in range(KC):
            now = i * KC + k
            for c in loads[now] if now < len(loads) else ():
                c.wait()
            for c in loads[now + AHEAD] if now + AHEAD < len(loads) else ():
                c.start()
            for d in range(2):
                at = pl.ds(m * rows + lo + d * n // 2, n // 2)
                product = jnp.dot(
                    x_rows(k, m, lo + d * n // 2, n // 2), wbuf[k],
                    preferred_element_type=jnp.float32,
                )
                if k == 0:
                    acc[s, at] = product
                else:
                    acc[s, at] += product
            if i == len(pieces) - 1:
                w_copy(2, k).start()
            if i > 0 and k == (3 if n == quarter else 2):
                add_piece(*pieces[i - 1])

        if i == 0:
            pl.semaphore_wait(barrier, 2)

        @pl.when(lane == 1 - m)
        def _():
            piece_copy(s, m, lo, n).start()

    for q in range(2):
        piece_copy(0, 0, q * quarter, quarter).wait_send()

    def step(s, carry):
        slot = lax.rem(s, 2)

        def own_two_back(f):
            @pl.when(is_peer(s - 2) == 0)
            def _():
                f(index(s - 2))

        def forward_behind(j):
            @pl.when(j >= LEAD + 1)
            def _():
                forward(j - LEAD - 1)

        for k in range(KC):
            w_copy(s, k).wait()
            for m in range(2):
                at = pl.ds(m * rows, rows)
                product = jnp.dot(
                    x_rows(k, m, 0, rows), wbuf[k], preferred_element_type=jnp.float32
                )
                if k == 0:
                    acc[slot, at] = product
                else:
                    acc[slot, at] += product

            @pl.when(s + 1 < steps)
            def _():
                w_copy(s + 1, k).start()

            if k == 1:
                pair_copy(s - 1).wait_send()

                @pl.when(s + lane >= 3)
                def _():
                    add_pair(s - 1)
            if k == 2:
                own_two_back(finish)
            if k == 3:
                own_two_back(send_total)
            if k == 4:
                own_two_back(forward_behind)

        pair_copy(s).start()
        return carry

    lax.fori_loop(2, steps, step, 0)

    for other in (sibling, across):
        pl.semaphore_signal(free_sem, inc=1, device_id=other, device_id_type=MESH)

    def landed(j, carry):
        y_pair(h_one, j).wait_recv()
        fwd_copy(h_one, j).wait_recv()
        return carry

    lax.fori_loop(0, early, landed, 0)
    bulk = [
        back_copy(h, y, owner, 0, early, back_sem.at[m, owner])
        for m, (h, y) in enumerate(((h_one, y_one), (h_two, y_two)))
        for owner in range(2)
    ]
    for c in bulk:
        c.start()

    last = np_ - 1
    pair_copy(steps - 1).wait_send()
    add_pair(steps - 1)
    for j in range(np_ - 2 - LEAD - 1, last - LEAD):
        forward(j)
    finish(last - 1)
    send_total(last - 1)
    forward(last - LEAD - 1 + 1)
    finish(last)
    pl.semaphore_wait(free_sem, 2)

    cut = rows // LAST

    def last_across(y, i):
        at = pl.ds(i * cut, cut)
        return pltpu.make_async_remote_copy(
            total.at[last % n_total, at], y.at[at, columns(chip, last)],
            y_send.at[last % n_total], last_recv.at[i],
            device_id=across, device_id_type=MESH,
        )

    def last_fwd(y, i):
        ref = y.at[pl.ds(i * cut, cut), columns(1 - chip, last)]
        return pltpu.make_async_remote_copy(
            ref, ref, fwd_send.at[last], fwd_recv.at[last],
            device_id=sibling, device_id_type=MESH,
        )

    def send_last(h, y):
        for i in range(LAST):
            last_across(y, i).start()
        y_pair(y, last).start()
        y[:, columns(chip, last)] = total[last % n_total]

    by_lane(send_last)

    for j in range(np_ - n_total, last):
        y_here(h_one, j).wait()
    by_lane(lambda h, y: back_copy(h, y, chip, early, LATE - 1, late_sem.at[0]).start())
    for j in range(early, np_):
        y_pair(h_one, j).wait_recv()
    by_lane(
        lambda h, y: back_copy(h, y, chip, early, LATE - 1, late_sem.at[1]).start(), 1 - lane
    )

    for j in range(last - LEAD + 1, last):
        forward(j)
    by_lane(lambda h, y: back_copy(h, y, 1 - chip, early, LATE - 1, late_sem.at[2]).start())
    for j in range(early, last):
        fwd_copy(h_one, j).wait_recv()
    by_lane(
        lambda h, y: back_copy(h, y, 1 - chip, early, LATE - 1, late_sem.at[3]).start(), 1 - lane
    )
    for i in range(LAST):
        last_across(y_one, i).wait_recv()
        by_lane(lambda h, y: last_fwd(y, i).start())

    for c in bulk:
        c.wait()
    for a in range(4):
        back_copy(h_one, y_one, 0, early, LATE - 1, late_sem.at[a]).wait()
    for j in range(np_ - n_part, np_):
        part_copy(j).wait_send()
    for j in range(np_ - n_total, np_):
        y_across(h_one, j).wait_send()
        y_pair(h_one, j).wait_send()

    def sent(j, carry):
        fwd_copy(h_one, j).wait_send()
        return carry

    lax.fori_loop(0, np_, sent, 0)
    fwd_copy(y_one, last).wait_recv()


def to_result(a, b, y_one, y_two, sem):
    rows = a.shape[0] // PIECES
    copies = [
        pltpu.make_async_copy(
            src.at[pl.ds(i * rows, rows)], dst.at[pl.ds(i * rows, rows)], sem.at[m, i]
        )
        for i in range(PIECES)
        for m, (src, dst) in enumerate(((a, y_one), (b, y_two)))
    ]
    for c in copies:
        c.start()
    for c in copies:
        c.wait()


def solution(mesh):
    def per_device(x_one, x_two, w_down):
        rows, width = x_one.shape
        cols = w_down.shape[1]
        blocks = cols // BN // 2
        n_part, n_peer, n_total = LEAD + 2, 2 * LEAD + 2, LEAD + 2
        dma = pltpu.SemaphoreType.DMA
        out = jax.ShapeDtypeStruct((rows, cols), jnp.bfloat16)
        hbm = pl.BlockSpec(memory_space=pltpu.HBM)
        vmem = pl.BlockSpec(memory_space=pltpu.VMEM)
        y_one, y_two = pl.pallas_call(
            kernel,
            out_shape=(out, out, out, out),
            in_specs=[hbm] * 3,
            out_specs=(vmem, vmem, hbm, hbm),
            scratch_shapes=[
                pltpu.VMEM((KC, width // KC, BN), jnp.bfloat16),
                pltpu.VMEM((2, 2 * rows, BN), jnp.float32),
                pltpu.VMEM((2, rows, BN), jnp.float32),
                pltpu.VMEM((n_part, rows, BN), jnp.float32),
                pltpu.VMEM((2, rows, BN), jnp.float32),
                pltpu.VMEM((n_peer, rows, BN), jnp.float32),
                pltpu.VMEM((n_total, rows, BN), jnp.bfloat16),
                dma((2, 2, KC)),
                dma((KC,)),
                dma((2,)),
                dma((2,)),
                dma((n_part,)),
                dma((n_peer,)),
                dma((n_total,)),
                dma((n_total,)),
                dma((blocks,)),
                dma((n_total,)),
                dma((blocks,)),
                dma((blocks,)),
                dma((blocks,)),
                dma((2, 2)),
                dma((4,)),
                dma((2,)),
                dma((2,)),
                dma((LAST,)),
                pltpu.SemaphoreType.REGULAR,
            ],
            compiler_params=pltpu.CompilerParams(
                collective_id=0, has_side_effects=True, vmem_limit_bytes=24 * 1024 * 1024
            ),
            cost_estimate=pl.CostEstimate(
                flops=4 * rows * width * cols,
                bytes_accessed=2 * width * cols,
                transcendentals=0,
            ),
        )(x_one, x_two, w_down)[:2]
        return pl.pallas_call(
            to_result,
            out_shape=(out, out),
            in_specs=[vmem] * 2,
            out_specs=(hbm, hbm),
            scratch_shapes=[dma((2, PIECES))],
            compiler_params=pltpu.CompilerParams(vmem_limit_bytes=1024 * 1024),
            cost_estimate=pl.CostEstimate(
                flops=0, bytes_accessed=8 * rows * cols, transcendentals=0
            ),
        )(y_one, y_two)

    return jax.shard_map(
        per_device,
        mesh=mesh,
        in_specs=(P("data", "tp"), P("data", "tp"), P("tp", None)),
        out_specs=(P("data", None), P("data", None)),
        check_vma=False,
    )
```
